256 devices in a mesh: dp: 8 (over z), expert: 4 (over y), tensor: 8 (over x, core).
Axes of the slice: x: 4, y: 4, z: 8, core: 2. Of those that a mesh axis runs over, the one named last changes fastest.
Arguments:
- tokens: bfloat16 [1024, 6144], P('dp', 'tensor'), may hold values from -6 to 6
- out_grad: bfloat16 [1024, 6144], P('dp', 'tensor'), may hold values from -6 to 6
- router_weight: bfloat16 [6144, 4], P('tensor'), may hold values from -0.078125 to 0.078125
- gate_weight: bfloat16 [4, 6144, 8192], P('expert', 'tensor', 'dp'), may hold values from -0.078125 to 0.078125
- up_weight: bfloat16 [4, 6144, 8192], P('expert', 'tensor', 'dp'), may hold values from -0.078125 to 0.078125
- down_weight: bfloat16 [4, 8192, 6144], P('expert', 'dp', 'tensor'), may hold values from -0.0625 to 0.0625
- expert_index: int32 [1024, 2], P('dp'), may hold values from 0 to 3, as said below
- slot_index: int32 [1024, 2], P('dp'), may hold values from 0 to 95, as said below
Outputs:
- tokens_grad: bfloat16 [1024, 6144], P(('dp', 'expert'), 'tensor')
- router_grad: float32 [6144, 4], P('tensor')
- gate_grad: bfloat16 [4, 6144, 8192], P('expert', 'tensor', 'dp')
- up_grad: bfloat16 [4, 6144, 8192], P('expert', 'tensor', 'dp')
- down_grad: bfloat16 [4, 8192, 6144], P('expert', 'dp', 'tensor')
The draws below stay inside these ranges and needn't reach their ends.
Inputs may be any that keep to these rules, and one draw needn't show every extreme that they name: `expert_index`: each row names two different experts; in each aligned block of 128 rows no expert is named more than 96 times, and one expert is named exactly 96 times in every block. `slot_index`: entry k of a row is a slot of the expert in entry k of the same row of expert_index; within one aligned block of 128 rows the choices of one expert have distinct slots.
All inputs are finite; a program needn't handle non-finite values.
Results may differ from the reference program's by a relative error of at most 0.025.
Values may be sent and summed in bfloat16 or wider, within the bound.
No kernel may reach another device: no remote copies, remote signals or barrier semaphores. Data moves between devices by JAX's collectives and lax.ppermute only.
A program may use at most 64 MiB of HBM per device.

```python
from functools import partial
import jax
import jax.numpy as jnp
from jax import lax

D = 6144
FF = 8192
EXPERTS = 4
TOK_DEV = 128
CAP = 96
TOKENS = 1024
SLOTS = 768
N_TENSOR = 8


def routing_block(block_key, busiest):
    load_key, order_key, token_key, swap_key, slot_key = jax.random.split(block_key, 5)
    shares = jax.random.randint(load_key, (EXPERTS - 1,), 1, 4)
    rest_picks = 2 * TOK_DEV - CAP
    other_loads = rest_picks * shares // jnp.sum(shares)
    leftover = rest_picks - jnp.sum(other_loads)
    other_loads = other_loads.at[jnp.argmin(shares)].add(leftover)
    others = (busiest + 1 + jax.random.permutation(order_key, EXPERTS - 1)) % EXPERTS
    expert_order = jnp.concatenate([jnp.reshape(busiest, (1,)), others]).astype(jnp.int32)
    run_counts = jnp.concatenate([jnp.array([CAP], jnp.int32), other_loads.astype(jnp.int32)])
    run_ends = jnp.cumsum(run_counts)
    run_starts = run_ends - run_counts
    pick_ids = jnp.arange(2 * TOK_DEV, dtype=jnp.int32)
    pick_run = jnp.sum((pick_ids[:, None] >= run_ends[None, :]).astype(jnp.int32), axis=1)
    pick_expert = expert_order[pick_run]
    pick_offset = pick_ids - run_starts[pick_run]
    tables = jax.vmap(partial(jax.random.permutation, x=CAP))(jax.random.split(slot_key, EXPERTS))
    pick_slot = tables[pick_expert, pick_offset]
    token_order = jax.random.permutation(token_key, TOK_DEV)
    first_pick = token_order
    second_pick = token_order + TOK_DEV
    expert_pair = jnp.stack([pick_expert[first_pick], pick_expert[second_pick]], axis=1)
    slot_pair = jnp.stack([pick_slot[first_pick], pick_slot[second_pick]], axis=1)
    swap_pair = jax.random.randint(swap_key, (TOK_DEV, 1), 0, 2) == 1
    expert_pair = jnp.where(swap_pair, expert_pair[:, ::-1], expert_pair)
    slot_pair = jnp.where(swap_pair, slot_pair[:, ::-1], slot_pair)
    return (expert_pair, slot_pair)


def make_routes(key):
    base_key = jax.random.fold_in(key, 7)
    row_blocks = TOKENS // TOK_DEV
    busiest = jax.random.randint(jax.random.fold_in(base_key, 1), (), 0, EXPERTS).astype(jnp.int32)
    block_keys = jax.random.split(jax.random.fold_in(base_key, 2), row_blocks)
    expert_pair, slot_pair = jax.vmap(partial(routing_block, busiest=busiest))(block_keys)
    return (expert_pair.reshape(TOKENS, 2).astype(jnp.int32), slot_pair.reshape(TOKENS, 2).astype(jnp.int32))


def draw_expert_index(key, part):
    return make_routes(key)[0]


def draw_slot_index(key, part):
    return make_routes(key)[1]


def shard_levels(stream_key, dims, cuts, smallest, largest):
    loudness = 1.0
    for position, parts in cuts:
        heights = jax.random.uniform(jax.random.fold_in(jax.random.fold_in(stream_key, 6), position), (parts,), jnp.float32, smallest / len(cuts), largest / len(cuts))
        loudness = loudness * jnp.repeat(jnp.exp(heights), dims[position] // parts).reshape((-1,) + (1,) * (len(dims) - 1 - position))
    return loudness


def normal_values(stream_key, dims, scale, reach, pieces=(), kind=jnp.bfloat16):
    entries = scale * jax.random.normal(stream_key, dims, jnp.float32)
    if pieces:
        entries = entries * shard_levels(stream_key, dims, pieces, -0.22, 0.18)
    return jnp.clip(entries, -reach, reach).astype(kind)


def setup_inputs(seed: int = 0) -> dict:
    key_list = jax.random.split(jax.random.key(seed), 9)
    tokens = normal_values(key_list[0], (TOKENS, D), 1.0, 6.0, ((0, 8), (1, 8)))
    out_grad = normal_values(key_list[1], (TOKENS, D), 1.0, 6.0, ((0, 8), (1, 8)))
    router_weight = normal_values(key_list[2], (D, EXPERTS), D ** -0.5, 0.078125, ((0, 8),))
    gate_weight = normal_values(key_list[3], (EXPERTS, D, FF), D ** -0.5, 0.078125, ((0, 4), (1, 8), (2, 8)))
    up_weight = normal_values(key_list[4], (EXPERTS, D, FF), D ** -0.5, 0.078125, ((0, 4), (1, 8), (2, 8)))
    down_weight = normal_values(key_list[5], (EXPERTS, FF, D), FF ** -0.5, 0.0625, ((0, 4), (1, 8), (2, 8)))
    expert_index = draw_expert_index(jax.random.fold_in(key_list[8], 71), 0)
    slot_index = draw_slot_index(jax.random.fold_in(key_list[8], 71), 0)
    return dict(tokens=tokens, out_grad=out_grad, router_weight=router_weight, gate_weight=gate_weight, up_weight=up_weight, down_weight=down_weight, expert_index=expert_index, slot_index=slot_index)


highest = lax.Precision.HIGHEST


def block_sum(left_side, right_side):
    block_width = D // N_TENSOR
    running = jnp.zeros((left_side.shape[0], right_side.shape[1]), jnp.float32)
    for row_block in range(N_TENSOR):
        partial_value = jnp.dot(left_side[:, row_block * block_width:(row_block + 1) * block_width], right_side[row_block * block_width:(row_block + 1) * block_width], preferred_element_type=jnp.float32)
        partial_value = lax.optimization_barrier(partial_value.astype(jnp.bfloat16)).astype(jnp.float32)
        running = running + partial_value
    return running


def expert_backward(operands):
    slot_tokens, slot_grads, slot_prob, gate_w, up_w, down_w = operands
    gate_sum = block_sum(slot_tokens, gate_w)
    up_sum = block_sum(slot_tokens, up_w)
    grad_act = block_sum(slot_grads, down_w.T)
    gate_sigmoid = jax.nn.sigmoid(gate_sum)
    hidden = (gate_sum * gate_sigmoid * up_sum).astype(jnp.bfloat16)
    prob_grad = jnp.sum(hidden.astype(jnp.float32) * grad_act, axis=1)
    act_grad = slot_prob.astype(jnp.float32)[:, None] * grad_act
    grad_gate = (act_grad * up_sum * gate_sigmoid * (1.0 + gate_sum * (1.0 - gate_sigmoid))).astype(jnp.bfloat16)
    grad_up = (act_grad * gate_sum * gate_sigmoid).astype(jnp.bfloat16)
    scaled_grads = (slot_prob.astype(jnp.float32)[:, None] * slot_grads.astype(jnp.float32)).astype(jnp.bfloat16)
    down_grad = jnp.dot(hidden.T, scaled_grads, preferred_element_type=jnp.float32).astype(jnp.bfloat16)
    gate_grad = jnp.dot(slot_tokens.T, grad_gate, preferred_element_type=jnp.float32).astype(jnp.bfloat16)
    up_grad = jnp.dot(slot_tokens.T, grad_up, preferred_element_type=jnp.float32).astype(jnp.bfloat16)
    slot_dx = jnp.dot(grad_gate, gate_w.T, preferred_element_type=jnp.float32) + jnp.dot(grad_up, up_w.T, preferred_element_type=jnp.float32)
    return slot_dx, prob_grad, gate_grad, up_grad, down_grad


def reference(tokens, out_grad, router_weight, gate_weight, up_weight, down_weight, expert_index, slot_index):
    logits = jnp.dot(tokens, router_weight, preferred_element_type=jnp.float32)
    chosen = jnp.take_along_axis(logits, expert_index, axis=1)
    pick_prob = jnp.stack([jax.nn.sigmoid(chosen[:, 0] - chosen[:, 1]), jax.nn.sigmoid(chosen[:, 1] - chosen[:, 0])], axis=1)
    prob_low = pick_prob.astype(jnp.bfloat16)
    row_block = (jnp.arange(TOKENS, dtype=jnp.int32) // TOK_DEV).astype(jnp.int32)
    slot_place = ((expert_index * (TOKENS // TOK_DEV) + row_block[:, None]) * CAP + slot_index).astype(jnp.int32)
    flat_place = slot_place.reshape(-1)
    slot_tokens = jnp.zeros((EXPERTS * SLOTS, D), jnp.bfloat16).at[flat_place].set(jnp.repeat(tokens, 2, axis=0))
    slot_grads = jnp.zeros((EXPERTS * SLOTS, D), jnp.bfloat16).at[flat_place].set(jnp.repeat(out_grad, 2, axis=0))
    slot_prob = jnp.zeros((EXPERTS * SLOTS,), jnp.bfloat16).at[flat_place].set(prob_low.reshape(-1))
    slot_dx, prob_grad, gate_grad, up_grad, down_grad = lax.map(expert_backward, (slot_tokens.reshape(EXPERTS, SLOTS, D), slot_grads.reshape(EXPERTS, SLOTS, D), slot_prob.reshape(EXPERTS, SLOTS), gate_weight, up_weight, down_weight))
    pick_dx = slot_dx.reshape(EXPERTS * SLOTS, D)[slot_place]
    pick_grad = prob_grad.reshape(-1)[slot_place]
    mixed_grad = jnp.sum(pick_prob * pick_grad, axis=1, keepdims=True)
    weights = pick_prob * (pick_grad - mixed_grad)
    onehot = (expert_index[:, :, None] == jnp.arange(EXPERTS, dtype=jnp.int32)[None, None, :]).astype(jnp.float32)
    logit_grad = jnp.sum(onehot * weights[:, :, None], axis=1)
    tokens_grad = (jnp.sum(pick_dx, axis=1) + jnp.dot(logit_grad, router_weight.astype(jnp.float32).T, precision=highest)).astype(jnp.bfloat16)
    router_grad = jnp.dot(tokens.astype(jnp.float32).T, logit_grad, precision=highest)
    return tokens_grad, router_grad, gate_grad, up_grad, down_grad
```

```python
import functools

import jax
import jax.numpy as jnp
from jax import lax
from jax.experimental import pallas as pl
from jax.experimental.pallas import tpu as pltpu
from jax.sharding import PartitionSpec as P

CAP = 96
CHUNKS = ((1, 2), (3, 4))
BF = jnp.bfloat16
F32 = jnp.float32
RING = 8
EXT = 128
D = 768
FF = 1024
WIDE = 3 * FF
COLS = WIDE + EXT
PACK = 2 * D + EXT
BACK = D + EXT


def sign_of(t):
    return 1 - 2 * (t % 2)


WITH = [(r * 8 + t, ((r + sign_of(t)) % RING) * 8 + t) for r in range(RING) for t in range(8)]
AGAINST = [(r * 8 + t, ((r - sign_of(t)) % RING) * 8 + t) for r in range(RING) for t in range(8)]
UP = [(r, (r + 1) % RING) for r in range(RING)]
DOWN = [(r, (r - 1) % RING) for r in range(RING)]
SWAP = [(t, t ^ 1) for t in range(8)]
PAIR_1 = [(t, ((t // 2) ^ (1 + 2 * (t % 2))) * 2 + t % 2) for t in range(8)]
PAIR_2 = [(t, ((t // 2) ^ (3 - 2 * (t % 2))) * 2 + t % 2) for t in range(8)]


def along_z(a, perm):
    return lax.ppermute(a, ("dp", "tensor"), perm)


def dot(a, b, ca, cb):
    return lax.dot_general(a, b, (((ca,), (cb,)), ((), ())), preferred_element_type=F32)


def split(v):
    high = v.astype(BF).astype(F32)
    return high, v - high


def call(kernel, outs, *args, scratch=(), name=None):
    single = not isinstance(outs, list)
    shapes = [jax.ShapeDtypeStruct(s, t) for s, t in ([outs] if single else outs)]
    vmem = pl.BlockSpec(memory_space=pltpu.VMEM)
    got = pl.pallas_call(
        kernel,
        out_shape=shapes,
        in_specs=[vmem] * len(args),
        out_specs=[vmem] * len(shapes),
        scratch_shapes=list(scratch),
        name=name,
    )(*args)
    return got[0] if single else got


def blocks(count, width, body):
    @pl.loop(0, count)
    def _(i):
        body(pl.ds(pl.multiple_of(i * width, width), width))


def ext_lanes(rows, columns):
    lane = lax.broadcasted_iota(jnp.int32, (rows, EXT), 1)
    out = jnp.zeros((rows, EXT), F32)
    for k, v in enumerate(columns):
        out = jnp.where(lane == k, v, out)
    return out.astype(BF)


def pair_total(a, b):
    e = a.astype(F32) + b.astype(F32)
    return e[:, 0:1] + e[:, 1:2]


def is_north():
    return lax.axis_index("tensor") % 2 == 0


def build_kernel(tok, grd, rwt, ei, si, t1, t2, sel_1, sel_2):
    t = lax.axis_index("tensor")
    x, core = t // 2, t % 2
    expert_id = lax.axis_index("expert")
    e0, e1, s0, s1 = ei[0:1, :], ei[1:2, :], si[0:1, :], si[1:2, :]
    logits = dot(rwt[...], tok[...], 1, 1)
    which = lax.broadcasted_iota(jnp.int32, logits.shape, 0)
    other = jnp.where(e0 == expert_id, e1, e0)
    sign = (which == expert_id).astype(F32) - (which == other).astype(F32)
    diff = jnp.sum(logits * sign, axis=0, keepdims=True)
    pos = lax.broadcasted_iota(jnp.int32, (CAP, 128), 0)
    b1 = pos >= 48
    rest = jnp.where(b1, pos - 48, pos)
    b2 = rest >= 24
    rest = jnp.where(b2, rest - 24, rest)
    for basis, out, sel_out in ((core, t1, sel_1), (1 - core, t2, sel_2)):
        owner = x ^ jnp.where(b1, 1 + 2 * basis, 0) ^ jnp.where(b2, 3 - 2 * basis, 0)
        order = owner * 24 + rest
        hit = ((e0 == expert_id) & (s0 == order)) | ((e1 == expert_id) & (s1 == order))
        wide = jnp.where(hit, 1.0, 0.0)
        sel = wide.astype(BF)
        sel_out[...] = sel
        out[:, :D] = dot(sel, tok[...], 1, 0).astype(BF)
        out[:, D : 2 * D] = dot(sel, grd[...], 1, 0).astype(BF)
        out[:, 2 * D :] = ext_lanes(CAP, split(jnp.sum(wide * diff, axis=1, keepdims=True)))


def product_kernel(units, *refs):
    nu = len(units)
    rows = nu * CAP
    firsts, seconds, refs = refs[:nu], refs[nu : 2 * nu], refs[2 * nu :]
    me_1 = me_2 = None
    if 4 in units:
        me_1, me_2, refs = refs[0], refs[1], refs[2:]
    wg, wu, wd, give, own, xc = refs

    def put(half, k, src):
        for b in range(4):
            at = half * rows + (b * nu + k) * 24
            xc[at : at + 24, :] = src[b * 24 : b * 24 + 24, :]

    for k, u in enumerate(units):
        if u == 4:
            north = is_north()

            @pl.when(north)
            def _():
                put(0, k, seconds[k])
                put(1, k, me_1)

            @pl.when(jnp.logical_not(north))
            def _():
                put(0, k, me_2)
                put(1, k, firsts[k])
        else:
            put(0, k, seconds[k])
            put(1, k, firsts[k])
    give[:, WIDE:] = xc[:rows, 2 * D :]
    own[:, WIDE:] = xc[rows:, 2 * D :]

    def store(v, k, c):
        v = v.astype(BF)
        at = pl.ds(pl.multiple_of(k * FF + c.start, 256), 256)
        give[:, at] = v[:rows]
        own[:, at] = v[rows:]

    def body(c):
        store(dot(xc[:, :D], wg[:, c], 1, 0), 0, c)
        store(dot(xc[:, :D], wu[:, c], 1, 0), 1, c)
        store(dot(xc[:, D : 2 * D], wd[c, :], 1, 1), 2, c)

    blocks(FF // 256, 256, body)


def halve_kernel(a, b, send, keep):
    n = send.shape[0]

    def body(c):
        v = (a[:, c].astype(F32) + b[:, c].astype(F32)).astype(BF)
        keep[:, c] = v[:n]
        send[:, c] = v[n:]

    blocks(WIDE // 256, 256, body)
    v = ext_lanes(2 * n, split(pair_total(a[:, WIDE:], b[:, WIDE:])))
    keep[:, WIDE:] = v[:n]
    send[:, WIDE:] = v[n:]


def hidden_kernel(a, b, share, acc):
    n = share.shape[0]
    prob = jax.nn.sigmoid(pair_total(a[:, WIDE:], b[:, WIDE:]))
    prob_low = prob.astype(BF).astype(F32)
    acc[...] = jnp.zeros_like(acc)

    @pl.loop(0, FF // 128)
    def _(i):
        cs = [pl.ds(pl.multiple_of(k * FF + i * 128, 128), 128) for k in range(3)]
        gate, up, grad = (a[:, c].astype(F32) + b[:, c].astype(F32) for c in cs)
        g = jax.nn.sigmoid(gate)
        hidden = (gate * g * up).astype(BF)
        acc[...] += hidden.astype(F32) * grad
        scaled = prob_low * grad
        share[:, cs[0]] = hidden
        share[:, cs[1]] = (scaled * up * g * (1.0 + gate * (1.0 - g))).astype(BF)
        share[:, cs[2]] = (scaled * gate * g).astype(BF)

    dprob = jnp.sum(acc[...], axis=1, keepdims=True)
    share[:, WIDE:] = ext_lanes(n, (*split(dprob), *split(prob)))


def join_kernel(a, b, out):
    n = a.shape[0]

    def body(c):
        out[:n, c] = a[:, c]
        out[n:, c] = b[:, c]

    blocks(COLS // 640, 640, body)


def dx_kernel(units, mine, theirs, wg, wu, *refs):
    nu = len(units)
    rows = nu * CAP
    *outs, acc = refs

    def body(c):
        v = 0.0
        for k, w in ((1, wg), (2, wu)):
            at = slice(k * FF, (k + 1) * FF)
            v = v + dot(jnp.concatenate([mine[:, at], theirs[:, at]], axis=0), w[c, :], 1, 1)
        acc[:, c] = v.astype(BF)

    blocks(D // 256, 256, body)

    def put(out, src, base, k):
        for b in range(4):
            at = (b * nu + k) * 24
            out[b * 24 : b * 24 + 24, :D] = acc[base + at : base + at + 24, :]
            out[b * 24 : b * 24 + 24, D:] = src[at : at + 24, WIDE:]

    for k, u in enumerate(units):
        a, b = outs[2 * k], outs[2 * k + 1]
        if u == 4:
            north = is_north()

            @pl.when(north)
            def _():
                put(a, mine, 0, k)
                put(b, theirs, rows, k)

            @pl.when(jnp.logical_not(north))
            def _():
                put(a, theirs, rows, k)
                put(b, mine, 0, k)
        else:
            put(a, mine, 0, k)
            put(b, theirs, rows, k)


def far_kernel(a, b, got, f, s):
    north = is_north().astype(F32)
    for out, v, w in ((f, a, 1.0 - north), (s, b, north)):
        out[:, :D] = (v[:, :D].astype(F32) + w * got[:, :D].astype(F32)).astype(BF)
        out[:, D:] = ext_lanes(CAP, split(pair_total(v[:, D:], w * got[:, D:].astype(F32))))


def back_kernel(a, b, got_a, got_b, f, s):
    for out, v, got in ((f, a, got_a), (s, b, got_b)):
        out[:, :D] = (v[:, :D].astype(F32) + got[:, :D].astype(F32)).astype(BF)
        out[:, D:] = ext_lanes(CAP, split(pair_total(v[:, D:], got[:, D:])))


def token_kernel(f, s, me, sel_1, sel_2, send):
    north = is_north().astype(F32)
    sel_me = (north * sel_1[...].astype(F32) + (1.0 - north) * sel_2[...].astype(F32)).astype(BF)
    sel = jnp.concatenate([sel_1[...], sel_2[...], sel_me], axis=0)
    back = jnp.concatenate([f[...], s[...], me[...]], axis=0)
    v = dot(sel, back[:, :D], 0, 0).astype(BF)
    ext = dot(back[:, D:], sel, 0, 0)
    high, low = split(ext[0:1] + ext[1:2])
    small = jnp.concatenate([high, low, ext[2:4], jnp.zeros((28, 128), F32)], axis=0).astype(BF)
    for k in range(4):
        send[k, :, :D] = v[k * 32 : k * 32 + 32]
        send[k, :, D:] = small


def out_kernel(got, tok, rwt, tokens_grad, router, scratch):
    total = got[0, :, :D].astype(F32)
    for k in range(1, 4):
        total = total + got[k, :, :D].astype(F32)
    small = [got[k, :, D:].astype(F32) for k in range(4)]
    pg = jnp.concatenate([v[0:1] + v[1:2] for v in small], axis=0)
    pp = jnp.concatenate([v[2:3] + v[3:4] for v in small], axis=0)
    logit_grad = pp * (pg - jnp.sum(pp * pg, axis=0, keepdims=True))
    high, low = (v.astype(BF) for v in split(logit_grad))
    scratch[...] = dot(high, rwt[...], 0, 0) + dot(low, rwt[...], 0, 0)
    at = pl.multiple_of(lax.axis_index("expert") * 32, 32)
    tokens_grad[...] = (total + scratch[pl.ds(at, 32), :]).astype(BF)
    part = dot(high, tok[...], 1, 0) + dot(low, tok[...], 1, 0)
    for k in range(RING):
        router[k] = part


def rows_of(refs, at):
    return jnp.concatenate([r[:, at] for r in refs], axis=0)


def wgrad_kernel(which, count, *refs):
    xs, theirs, mine = refs[:count], refs[count : 2 * count], refs[2 * count : 3 * count]
    out, xt = refs[3 * count :]
    xt[...] = rows_of(xs, slice(0, D)).T
    grads = [r for pair in zip(theirs, mine) for r in pair]

    def body(c):
        at = pl.ds(pl.multiple_of(which * FF + c.start, 256), 256)
        out[:, c] = dot(xt[...], rows_of(grads, at), 1, 0).astype(BF)

    blocks(FF // 256, 256, body)


def down_kernel(count, *refs):
    xs, theirs, mine = refs[:count], refs[count : 2 * count], refs[2 * count : 3 * count]
    out, ht, scaled = refs[3 * count :]
    both = [r for pair in zip(theirs, mine) for r in pair]
    ht[...] = rows_of(both, slice(0, FF)).T
    prob = rows_of(both, slice(WIDE, COLS)).astype(F32)[:, 2:3]
    scaled[...] = (prob * rows_of(xs, slice(D, 2 * D)).astype(F32)).astype(BF)

    def body(c):
        out[:, c] = dot(ht[...], scaled[:, c], 1, 0).astype(BF)

    blocks(D // 256, 256, body)


def shards(
    tokens, out_grad, router_weight, gate_weight, up_weight, down_weight, expert_index, slot_index
):
    wg, wu, wd = gate_weight[0], up_weight[0], down_weight[0]
    rwt = router_weight.T
    t1, t2, sel_1, sel_2 = call(
        build_kernel,
        [((CAP, PACK), BF)] * 2 + [((CAP, 128), BF)] * 2,
        tokens, out_grad, rwt, expert_index.T, slot_index.T,
        name="build",
    )

    first, second = {}, {}
    f, s = t1, t2
    for u in (1, 2, 3):
        f, s = along_z(f, AGAINST), along_z(s, WITH)
        first[u], second[u] = f, s
    far = lax.ppermute(jnp.where(lax.axis_index("tensor") % 2 == 0, s, f), "dp", UP)
    first[4] = second[4] = far

    dx_first, dx_second = {}, {}
    all_x, all_theirs, all_mine = [], [], []
    for units in CHUNKS:
        rows = len(units) * CAP
        extra = (t1, t2) if 4 in units else ()
        give, own, xc = call(
            functools.partial(product_kernel, units),
            [((rows, COLS), BF)] * 2 + [((2 * rows, PACK), BF)],
            *(first[u] for u in units), *(second[u] for u in units), *extra, wg, wu, wd,
            name="products",
        )
        got = lax.ppermute(give, "tensor", SWAP)
        half = [((rows // 2, COLS), BF)] * 2
        send, keep = call(halve_kernel, half, own, got, name="halve_1")
        got = lax.ppermute(send, "tensor", PAIR_1)
        half = [((rows // 4, COLS), BF)] * 2
        send, keep = call(halve_kernel, half, keep, got, name="halve_2")
        got = lax.ppermute(send, "tensor", PAIR_2)
        share = call(
            hidden_kernel, ((rows // 4, COLS), BF), keep, got,
            scratch=[pltpu.VMEM((rows // 4, 128), F32)], name="hidden",
        )
        got = lax.ppermute(share, "tensor", PAIR_2)
        pair = call(join_kernel, ((rows // 2, COLS), BF), share, got, name="join_2")
        got = lax.ppermute(pair, "tensor", PAIR_1)
        mine = call(join_kernel, ((rows, COLS), BF), pair, got, name="join_1")
        theirs = lax.ppermute(mine, "tensor", SWAP)
        outs = call(
            functools.partial(dx_kernel, units), [((CAP, BACK), BF)] * (2 * len(units)),
            mine, theirs, wg, wu, scratch=[pltpu.VMEM((2 * rows, D), BF)], name="dx",
        )
        for k, u in enumerate(units):
            dx_first[u], dx_second[u] = outs[2 * k], outs[2 * k + 1]
        all_x.append(xc)
        all_theirs.append(theirs)
        all_mine.append(mine)

    two = [((CAP, BACK), BF)] * 2
    got = lax.ppermute(dx_second[4], "dp", DOWN)
    f, s = call(far_kernel, two, dx_first[3], dx_second[3], got, name="far")
    for u in (2, 1):
        f, s = along_z(f, WITH), along_z(s, AGAINST)
        f, s = call(back_kernel, two, dx_first[u], dx_second[u], f, s, name="back")
    f, s = along_z(f, WITH), along_z(s, AGAINST)
    send = call(
        token_kernel, ((4, 32, BACK), BF), f, s, dx_first[4], sel_1, sel_2, name="to_tokens"
    )
    got = lax.all_to_all(send, "expert", 0, 0, tiled=True)
    tokens_grad, spread = call(
        out_kernel, [((32, D), BF), ((RING, 4, D), F32)], got, tokens, rwt,
        scratch=[pltpu.VMEM((128, D), F32)], name="outputs",
    )
    router_grad = lax.all_to_all(spread, "dp", 0, 0, tiled=True).sum(axis=0).T

    count = len(CHUNKS)
    slots = sum(len(units) for units in CHUNKS) * 2 * CAP
    operands = (*all_x, *all_theirs, *all_mine)
    gate_grad, up_grad = (
        call(
            functools.partial(wgrad_kernel, k, count), ((D, FF), BF), *operands,
            scratch=[pltpu.VMEM((D, slots), BF)], name="wgrad",
        )
        for k in (1, 2)
    )
    down_grad = call(
        functools.partial(down_kernel, count), ((FF, D), BF), *operands,
        scratch=[pltpu.VMEM((FF, slots), BF), pltpu.VMEM((slots, D), BF)], name="wgrad_down",
    )
    return (tokens_grad, router_grad, gate_grad[None], up_grad[None], down_grad[None])


def solution(mesh):
    in_specs = (
        P("dp", "tensor"),
        P("dp", "tensor"),
        P("tensor", None),
        P("expert", "tensor", "dp"),
        P("expert", "tensor", "dp"),
        P("expert", "dp", "tensor"),
        P("dp", None),
        P("dp", None),
    )
    out_specs = (
        P(("dp", "expert"), "tensor"),
        P("tensor", None),
        P("expert", "tensor", "dp"),
        P("expert", "tensor", "dp"),
        P("expert", "dp", "tensor"),
    )
    return jax.shard_map(shards, mesh=mesh, in_specs=in_specs, out_specs=out_specs, check_vma=False)
```
